8 devices in a mesh: rep: 1 (over z), dp: 8 (over x, y, core).
Axes of the slice: x: 2, y: 2, z: 1, core: 2. Of those that a mesh axis runs over, the one named last changes fastest.
Arguments:
- x: bfloat16 [8, 2048, 1024], P(('rep', 'dp'))
- dy: bfloat16 [8, 2048, 1024], P(('rep', 'dp'))
- w_gate: bfloat16 [2, 1024, 4096], replicated
- w_up: bfloat16 [2, 1024, 4096], replicated
- w_down: bfloat16 [2, 4096, 1024], replicated
- m_w_gate: float32 [2, 1024, 4096], replicated
- m_w_up: float32 [2, 1024, 4096], replicated
- m_w_down: float32 [2, 4096, 1024], replicated
- v_w_gate: float32 [2, 1024, 4096], replicated
- v_w_up: float32 [2, 1024, 4096], replicated
- v_w_down: float32 [2, 4096, 1024], replicated
Outputs:
- output 1: bfloat16 [2, 1024, 4096], P('rep')
- output 2: bfloat16 [2, 1024, 4096], P('rep')
- output 3: bfloat16 [2, 4096, 1024], P('rep')
- output 4: float32 [2, 1024, 4096], P('rep')
- output 5: float32 [2, 1024, 4096], P('rep')
- output 6: float32 [2, 4096, 1024], P('rep')
- output 7: float32 [2, 1024, 4096], P('rep')
- output 8: float32 [2, 1024, 4096], P('rep')
- output 9: float32 [2, 4096, 1024], P('rep')
All inputs are finite; a program needn't handle non-finite values.
Results may differ from the reference program's by a relative error of at most 0.022.
Values are sent between devices in bfloat16 or wider.
A program may use at most 2.75 GiB of HBM per device.

```python
import jax
import jax.numpy as jnp
from jax import lax

SEQUENCES = 8
TOKENS = 2048
D = 1024
FF = 4096
LAYERS = 2
NAMES = ("w_gate", "w_up", "w_down")
SHAPES = {"w_gate": (LAYERS, D, FF), "w_up": (LAYERS, D, FF), "w_down": (LAYERS, FF, D)}


def bump(key, n, height):
    away = (jnp.arange(n, dtype=jnp.int32) - jax.random.randint(key, (), 0, n, jnp.int32)) % n
    return jnp.where(away < n // 8, height, 1.0)


def together(key, own, strength):
    shared = jax.random.normal(key, own.shape[1:], jnp.float32)
    return (own + strength * shared) * lax.rsqrt(1 + strength * strength)


def setup_inputs(seed: int = 0, part: int = 0) -> dict:
    kx, kdy, ka, kb, kz, kf, kh, kl, *keys = jax.random.split(jax.random.key(seed), 8 + 3 * len(NAMES))
    kx, kdy, ka, kb = (jax.random.fold_in(k, part) for k in (kx, kdy, ka, kb))
    kw, km, kv = (keys[i::3] for i in range(3))
    shape = (SEQUENCES, TOKENS, D)
    much_x, much_dy = jax.random.uniform(kz, (2,), jnp.float32, 0.0, 1.0)
    loud = 2.0 ** jax.random.uniform(jax.random.fold_in(kz, 1), (), jnp.float32, -1.0, 2.0)
    layers = 2.0 ** jax.random.uniform(kl, (LAYERS, 1, 1), jnp.float32, -1.0, 1.0)
    x = together(ka, jax.random.normal(kx, shape, jnp.float32), much_x) * bump(kf, D, 4.0)
    dy = together(kb, jax.random.normal(kdy, shape, jnp.float32), much_dy)
    drawn = {"x": x.astype(jnp.bfloat16), "dy": (loud * dy * (SEQUENCES * TOKENS) ** -0.5).astype(jnp.bfloat16)}
    for key, name in zip(kw, NAMES, strict=True):
        w = jax.random.normal(key, SHAPES[name], jnp.float32) * SHAPES[name][1] ** -0.5
        drawn[name] = (w * {"w_gate": 1.0, "w_up": bump(kh, FF, 4.0), "w_down": layers}[name]).astype(jnp.bfloat16)
    for key, name in zip(km, NAMES, strict=True):
        drawn[f"m_{name}"] = 0.1 * jax.random.normal(key, SHAPES[name], jnp.float32)
    for key, name in zip(kv, NAMES, strict=True):
        drawn[f"v_{name}"] = jax.random.uniform(key, SHAPES[name], jnp.float32, 0.005, 0.015)
    return drawn


def matmul(a, w):
    return jnp.dot(a, w, preferred_element_type=jnp.float32).astype(jnp.bfloat16)


def normed(h):
    wide = h.astype(jnp.float32)
    scale = lax.rsqrt(jnp.mean(wide**2, -1, keepdims=True) + 1e-6)
    return (wide * scale).astype(jnp.bfloat16)


def layer(h, w):
    a = normed(h)
    gate = jnp.dot(a, w["w_gate"], preferred_element_type=jnp.float32)
    up = jnp.dot(a, w["w_up"], preferred_element_type=jnp.float32)
    return h + matmul((jax.nn.silu(gate) * up).astype(jnp.bfloat16), w["w_down"])


def adamw(w, m, v, g):
    m = 0.9 * m + 0.1 * g
    v = 0.95 * v + 0.05 * g * g
    step = m * lax.rsqrt(v + 1e-8) + 0.1 * w
    return (w - 0.02 * step).astype(jnp.bfloat16), m, v


def stack(weights, h):
    return lax.scan(lambda h, w: (layer(h, w), None), h, weights)[0]


def reference(x, dy, w_gate, w_up, w_down, m_w_gate, m_w_up, m_w_down, v_w_gate, v_w_up, v_w_down):
    weights = dict(zip(NAMES, (w_gate, w_up, w_down), strict=True))

    def take(so_far, sequence):
        h, by_y = sequence
        _, back = jax.vjp(lambda w: stack(w, h), weights)
        return jax.tree.map(lambda total, term: total + term.astype(jnp.float32), so_far, back(by_y)[0]), None

    none_yet = {name: jnp.zeros(w.shape, jnp.float32) for name, w in weights.items()}
    by_weights, _ = lax.scan(take, none_yet, (x, dy))
    gradients = [by_weights[name].astype(jnp.bfloat16).astype(jnp.float32) for name in NAMES]
    new = [
        adamw(w.astype(jnp.float32), m, v, g)
        for w, m, v, g in zip((w_gate, w_up, w_down), (m_w_gate, m_w_up, m_w_down), (v_w_gate, v_w_up, v_w_down), gradients, strict=True)
    ]
    return tuple(one[which] for which in range(3) for one in new)
```

```python
import functools

import jax
import jax.numpy as jnp
from jax import lax
from jax.experimental import pallas as pl
from jax.experimental.pallas import tpu as pltpu
from jax.sharding import PartitionSpec as P

F32, BF16 = jnp.float32, jnp.bfloat16
MESH = pl.DeviceIdType.MESH
H = 512
TB = 512
RING = 3
GROUPS = (8, 5, 3)


def dot(a, b, ca=1, cb=0):
    return lax.dot_general(a, b, (((ca,), (cb,)), ((), ())), preferred_element_type=F32)


def ds(i, n):
    return pl.ds(pl.multiple_of(i * n, n), n)


def step_kernel(
    x, dy, wg, wu, wd, shard, pq, acts, h1, a0t,
    a, at, c, ct, acc, wgu_v, wd_v, r0, r1, r2, k1, s1, k2, s2, sv, w_sem, in_sem, pq_sem, act_sem, sv_sem,
    send0, recv0, send1, recv1, send2, recv2, free0, free1, free2,
):
    tokens, d = x.shape
    ff = wd.shape[1]
    nc = ff // H
    nb = tokens // TB
    total = 2 * nc
    me = lax.axis_index("dp")
    mc, my, mx = me % 2, (me // 2) % 2, me // 4
    over_c, over_y, over_x = me + 1 - 2 * mc, me + 2 - 4 * my, me + 4 - 8 * mx
    barrier = pltpu.get_barrier_semaphore()
    for peer in (over_c, over_y, over_x):
        pl.semaphore_signal(barrier, inc=1, device_id={"dp": peer}, device_id_type=MESH)

    def weights(n):
        j, slot = n % nc, n % 2
        lay = jnp.where((n >= nc) & (n < 2 * nc), 1, 0)
        return (
            pltpu.make_async_copy(wd.at[lay, ds(j, H), :], wd_v.at[slot], w_sem.at[slot, 0]),
            pltpu.make_async_copy(wg.at[lay, :, ds(j, H)], wgu_v.at[slot, :, pl.ds(0, H)], w_sem.at[slot, 1]),
            pltpu.make_async_copy(wu.at[lay, :, ds(j, H)], wgu_v.at[slot, :, pl.ds(H, H)], w_sem.at[slot, 2]),
        )

    def pq_load(j, tb):
        return pltpu.make_async_copy(pq.at[j, ds(tb, TB), :], acc.at[ds(tb, TB), :], pq_sem.at[tb])

    def copy0(s, dwb):
        return pltpu.make_async_remote_copy(
            dwb.at[s % 2, :, 1 - mc], r0.at[s % 2], send0.at[s % 2], recv0.at[s], device_id={"dp": over_c}, device_id_type=MESH
        )

    def copy1(s, ab):
        return pltpu.make_async_remote_copy(
            s1.at[s % 2, ab], r1.at[s % RING, ab], send1.at[s % 2, ab], recv1.at[s, ab],
            device_id={"dp": (over_x, over_y)[ab]}, device_id_type=MESH,
        )

    def copy2(s, ab):
        return pltpu.make_async_remote_copy(
            s2.at[s % 2, ab], r2.at[s % RING, ab], send2.at[s % 2, ab], recv2.at[s, ab],
            device_id={"dp": (over_y, over_x)[ab]}, device_id_type=MESH,
        )

    def out_copy(s):
        return pltpu.make_async_copy(sv.at[s % 2], shard.at[s], sv_sem.at[s % 2])

    def send_own(s, dwb):
        @pl.when(s >= 2)
        def _():
            pl.semaphore_wait(free0, 1)

        copy0(s, dwb).start()

    def reduce1(s, dwb):
        copy0(s, dwb).wait()

        @pl.when(s >= 2)
        def _():
            for ab in range(2):
                copy1(s - 2, ab).wait_send()

        slot = s % 2

        def one(i, _):
            k, o = i // 2, i % 2
            for ab in range(2):
                rows = pl.ds(ab * 64, 64)
                keep = k * 4 + (mx * 2 + o if ab == 0 else o * 2 + my)
                give = k * 4 + ((1 - mx) * 2 + o if ab == 0 else o * 2 + 1 - my)
                k1[slot, ab, i] = dwb[slot, keep, mc, rows, :].astype(F32) + r0[slot, keep, rows, :].astype(F32)
                s1[slot, ab, i] = (dwb[slot, give, mc, rows, :].astype(F32) + r0[slot, give, rows, :].astype(F32)).astype(BF16)
            return 0

        lax.fori_loop(0, 6, one, 0)

        @pl.when(s + 2 < total)
        def _():
            pl.semaphore_signal(free0, inc=1, device_id={"dp": over_c}, device_id_type=MESH)

        @pl.when(s >= RING)
        def _():
            for ab in range(2):
                pl.semaphore_wait(free1.at[ab], 1)

        for ab in range(2):
            copy1(s, ab).start()

    def reduce2(s):
        slot, ring = s % 2, s % RING

        @pl.when(s >= 2)
        def _():
            for ab in range(2):
                copy2(s - 2, ab).wait_send()

        for ab in range(2):
            copy1(s, ab).wait_recv()

        def one(k, _):
            for ab in range(2):
                mine = (my, mx)[ab]
                keep, give = k * 2 + mine, k * 2 + 1 - mine
                k2[slot, ab, k] = k1[slot, ab, keep] + r1[ring, ab, keep].astype(F32)
                s2[slot, ab, k] = (k1[slot, ab, give] + r1[ring, ab, give].astype(F32)).astype(BF16)
            return 0

        lax.fori_loop(0, 3, one, 0)

        @pl.when(s + RING < total)
        def _():
            for ab in range(2):
                pl.semaphore_signal(free1.at[ab], inc=1, device_id={"dp": (over_x, over_y)[ab]}, device_id_type=MESH)

        @pl.when(s >= RING)
        def _():
            for ab in range(2):
                pl.semaphore_wait(free2.at[ab], 1)

        for ab in range(2):
            copy2(s, ab).start()

    def reduce3(s):
        slot, ring = s % 2, s % RING

        @pl.when(s >= 2)
        def _():
            out_copy(s - 2).wait()

        for ab in range(2):
            copy2(s, ab).wait_recv()

        def one(k, _):
            for ab in range(2):
                sv[slot, k, pl.ds(ab * 64, 64), :] = (k2[slot, ab, k] + r2[ring, ab, k].astype(F32)).astype(BF16)
            return 0

        lax.fori_loop(0, 3, one, 0)

        @pl.when(s + RING < total)
        def _():
            for ab in range(2):
                pl.semaphore_signal(free2.at[ab], inc=1, device_id={"dp": (over_y, over_x)[ab]}, device_id_type=MESH)

        out_copy(s).start()

    def when(cond, f, *args):
        @pl.when(cond)
        def _():
            f(*args)

    for w in weights(0):
        w.start()

    def forward(xb, stage, stage_act):
        loads = [pltpu.make_async_copy(x.at[ds(tb, TB), :], xb.at[ds(tb, TB), :], in_sem.at[tb]) for tb in range(nb)]
        dy_load = pltpu.make_async_copy(dy, c, in_sem.at[nb])
        for load in loads:
            load.start()
        dy_load.start()
        for load in loads:
            load.wait()

        def norm(tb, _):
            r = ds(tb, 256)
            wide = xb[r, :].astype(F32)
            scale = lax.rsqrt(jnp.mean(wide * wide, -1, keepdims=True) + 1e-6)
            a[r, :] = (wide * scale).astype(BF16)
            acc[r, :] = jnp.zeros((256, d), F32)
            return 0

        lax.fori_loop(0, tokens // 256, norm, 0)
        dy_load.wait()

        def stored(n):
            j, tb = n // nb, n % nb
            return (
                pltpu.make_async_copy(stage.at[n % 2], pq.at[j, ds(tb, TB), :], pq_sem.at[n % 2]),
                pltpu.make_async_copy(stage_act.at[n % 2], acts.at[j, ds(tb, TB), :], act_sem.at[n % 2]),
            )

        def chunk(j, _):
            slot = j % 2
            for w in weights(j + 1):
                w.start()
            for w in weights(j):
                w.wait()

            def block(tb, _):
                n = j * nb + tb
                r = ds(tb, TB)

                @pl.when(n >= 2)
                def _():
                    for store in stored(n - 2):
                        store.wait()

                gu = dot(a[r, :], wgu_v[slot])
                g, u = gu[:, :H], gu[:, H:]
                s = jax.nn.sigmoid(g)
                p = g * s
                act = (p * u).astype(BF16)
                stage[n % 2, :, :H] = p
                stage[n % 2, :, H:] = u * (s + p * (1 - s))
                stage_act[n % 2] = act
                acc[r, :] += dot(act, wd_v[slot])
                tr, tc = ds(n // 2, 128), ds(n % 2, d // 2)
                ct[tc, tr] = c[tr, tc].T
                at[tc, tr] = a[tr, tc].T
                for store in stored(n):
                    store.start()
                return 0

            lax.fori_loop(0, nb, block, 0)
            return 0

        lax.fori_loop(0, nc, chunk, 0)
        last = nc * nb
        for n in (last - 2, last - 1):
            for store in stored(n):
                store.wait()
        keep_at = pltpu.make_async_copy(at, a0t, in_sem.at[nb])
        keep_at.start()

        def finish(tb, _):
            r = ds(tb, 256)
            xb[r, :] = (xb[r, :].astype(F32) + acc[r, :].astype(BF16).astype(F32)).astype(BF16)
            wide = xb[r, :].astype(F32)
            scale = lax.rsqrt(jnp.mean(wide * wide, -1, keepdims=True) + 1e-6)
            a[r, :] = (wide * scale).astype(BF16)
            acc[r, :] = jnp.zeros((256, d), F32)
            return 0

        lax.fori_loop(0, tokens // 256, finish, 0)
        keep_h = pltpu.make_async_copy(xb, h1, in_sem.at[0])
        keep_h.start()
        keep_at.wait()

        def turn(tb, _):
            r = ds(tb, 256)
            at[:, r] = a[r, :].T
            return 0

        lax.fori_loop(0, tokens // 256, turn, 0)
        keep_h.wait()

    pl.run_scoped(
        forward, pltpu.VMEM((tokens, d), BF16), pltpu.VMEM((2, TB, 2 * H), F32), pltpu.VMEM((2, TB, H), BF16)
    )
    pl.semaphore_wait(barrier, 3)

    def backward(act, dgu, dwb):
        def gradients(s):
            slot = s % 2

            def half(xh, _):
                rows = ds(xh, d // 2)
                both = dot(at[rows, :], dgu[...]).astype(BF16)
                down = dot(ct[rows, :], act[...]).astype(BF16)
                for k, part in enumerate((both[:, :H], both[:, H:], down)):
                    for y in range(2):
                        for core in range(2):
                            dwb[slot, k * 4 + xh * 2 + y, core] = part[(y * 2 + core) * 128 : (y * 2 + core + 1) * 128]
                return 0

            lax.fori_loop(0, 2, half, 0)

        def chunk1(s, _):
            n = nc + s
            slot = n % 2
            for w in weights(n + 1):
                w.start()
            for w in weights(n):
                w.wait()

            def block(tb, _):
                r = ds(tb, TB)
                gu = dot(a[r, :], wgu_v[slot])
                dact = dot(c[r, :], wd_v[slot], 1, 1).astype(BF16).astype(F32)
                g, u = gu[:, :H], gu[:, H:]
                sg = jax.nn.sigmoid(g)
                p = g * sg
                act[r, :] = (p * u).astype(BF16)
                dgu[r, H:] = (dact * p).astype(BF16)
                dgu[r, :H] = (dact * (u * (sg + p * (1 - sg)))).astype(BF16)
                return 0

            lax.fori_loop(0, nb, block, 0)
            when(s == nc - 1, lambda: pltpu.make_async_copy(h1, a, in_sem.at[0]).start())
            when(s >= 2, reduce3, s - 2)
            gradients(s)
            send_own(s, dwb)
            when(s >= 1, reduce2, s - 1)

            def back(tb, _):
                r = ds(tb, TB)
                acc[r, :] += dot(dgu[r, :], wgu_v[slot], 1, 1)
                return 0

            lax.fori_loop(0, nb, back, 0)
            reduce1(s, dwb)
            return 0

        lax.fori_loop(0, nc, chunk1, 0)

        load_at = pltpu.make_async_copy(a0t, at, in_sem.at[1])
        load_at.start()
        pltpu.make_async_copy(h1, a, in_sem.at[0]).wait()

        def act_load(j):
            return pltpu.make_async_copy(acts.at[j], act, act_sem.at[0])

        act_load(0).start()
        for tb in range(nb):

            def norm_back(i, _):
                r = pl.ds(pl.multiple_of(tb * TB + i * 256, 256), 256)
                wide = a[r, :].astype(F32)
                scale = lax.rsqrt(jnp.mean(wide * wide, -1, keepdims=True) + 1e-6)
                da = acc[r, :].astype(BF16).astype(F32)
                inner = jnp.mean(da * wide, -1, keepdims=True)
                dh = (da * scale - wide * (inner * scale * scale * scale)).astype(BF16).astype(F32)
                dh = (c[r, :].astype(F32) + dh).astype(BF16)
                c[r, :] = dh
                ct[:, r] = dh.T
                return 0

            lax.fori_loop(0, TB // 256, norm_back, 0)
            pq_load(0, tb).start()
        load_at.wait()

        def chunk0(s, _):
            n = nc + s
            j, slot = s - nc, n % 2

            @pl.when(j + 1 < nc)
            def _():
                weights(n + 1)[0].start()

            weights(n)[0].wait()

            @pl.when(j == 0)
            def _():
                for w in weights(2 * nc)[1:]:
                    w.wait()

            def block(tb, _):
                r = ds(tb, TB)
                pq_load(j, tb).wait()
                dact = dot(c[r, :], wd_v[slot], 1, 1).astype(BF16).astype(F32)
                dgu[r, H:] = (dact * acc[r, :H]).astype(BF16)
                dgu[r, :H] = (dact * acc[r, H:]).astype(BF16)
                when(j + 1 < nc, lambda: pq_load(j + 1, tb).start())
                return 0

            lax.fori_loop(0, nb, block, 0)
            when(j >= 1, reduce1, s - 1, dwb)
            act_load(j).wait()
            gradients(s)
            when(j + 1 < nc, lambda: act_load(j + 1).start())
            send_own(s, dwb)

            @pl.when(j >= 1)
            def _():
                reduce2(s - 2)
                reduce3(s - 3)

            return 0

        lax.fori_loop(nc, 2 * nc, chunk0, 0)

        end = total - 1
        reduce1(end, dwb)
        reduce2(end - 1)
        reduce3(end - 2)
        reduce2(end)
        reduce3(end - 1)
        reduce3(end)
        for s in (end - 1, end):
            out_copy(s).wait()
            for ab in range(2):
                copy1(s, ab).wait_send()
                copy2(s, ab).wait_send()

    pl.run_scoped(
        backward,
        pltpu.VMEM((tokens, H), BF16),
        pltpu.VMEM((tokens, 2 * H), BF16),
        pltpu.VMEM((2, 12, 2, 128, H), BF16),
    )


def gradients_of(x, dy, wg, wu, wd):
    tokens, d = x.shape
    ff = wd.shape[1]
    nc, nb = ff // H, tokens // TB
    any_, vmem, dma = pl.BlockSpec(memory_space=pl.ANY), pltpu.VMEM, pltpu.SemaphoreType.DMA
    shapes = [
        ((2 * nc, 3, d // 8, H), BF16),
        ((nc, tokens, 2 * H), F32),
        ((nc, tokens, H), BF16),
        ((tokens, d), BF16),
        ((d, tokens), BF16),
    ]
    flops = 30 * tokens * d * ff
    return pl.pallas_call(
        step_kernel,
        name="train_step",
        out_shape=[jax.ShapeDtypeStruct(*one) for one in shapes],
        in_specs=[any_] * 5,
        out_specs=[any_] * 5,
        scratch_shapes=[
            vmem((tokens, d), BF16),
            vmem((d, tokens), BF16),
            vmem((tokens, d), BF16),
            vmem((d, tokens), BF16),
            vmem((tokens, d), F32),
            vmem((2, d, 2 * H), BF16),
            vmem((2, H, d), BF16),
            vmem((2, 12, 128, H), BF16),
            vmem((RING, 2, 6, 64, H), BF16),
            vmem((RING, 2, 3, 64, H), BF16),
            vmem((2, 2, 6, 64, H), F32),
            vmem((2, 2, 6, 64, H), BF16),
            vmem((2, 2, 3, 64, H), F32),
            vmem((2, 2, 3, 64, H), BF16),
            vmem((2, 3, 128, H), BF16),
            dma((2, 3)),
            dma((nb + 1,)),
            dma((nb,)),
            dma((2,)),
            dma((2,)),
            dma((2,)),
            dma((2 * nc,)),
            dma((2, 2)),
            dma((2 * nc, 2)),
            dma((2, 2)),
            dma((2 * nc, 2)),
            pltpu.SemaphoreType.REGULAR,
            pltpu.SemaphoreType.REGULAR((2,)),
            pltpu.SemaphoreType.REGULAR((2,)),
        ],
        compiler_params=pltpu.CompilerParams(collective_id=0, has_side_effects=True, vmem_limit_bytes=67_000_000),
        cost_estimate=pl.CostEstimate(flops=flops, bytes_accessed=300_000_000, transcendentals=0),
    )(x, dy, wg, wu, wd)[0]


def adam_kernel(gg, gu, gd, *refs):
    ins, outs = refs[:9], refs[-9:]
    rows = ins[0].shape[1]
    grads = (
        gg[...].reshape(rows, H),
        gu[...].reshape(rows, H),
        gd[...].reshape(gd.shape[0] * gd.shape[3], gd.shape[4]).astype(F32).T,
    )
    for i, g in enumerate(grads):
        g = g.astype(F32)
        w, m, v = ins[i][0].astype(F32), ins[3 + i][0], ins[6 + i][0]
        m = 0.9 * m + 0.1 * g
        v = 0.95 * v + 0.05 * g * g
        step = m * lax.rsqrt(v + 1e-8) + 0.1 * w
        outs[i][0] = (w - 0.02 * step).astype(BF16)
        outs[3 + i][0] = m
        outs[6 + i][0] = v


def adam(first, count, g, arrays, so_far):
    layers, d, ff = arrays[0].shape
    nc = ff // H

    def place(i):
        s = first + i
        return layers - 1 - s // nc, s % nc

    def wide(i, r):
        lay, j = place(i)
        return lay, r, j

    def tall(i, r):
        lay, j = place(i)
        return lay, j * 2 + r, 0

    g_wide = [pl.BlockSpec((4, 1, 1, 128, H), functools.partial(lambda i, r, k: (r, i, k, 0, 0), k=k)) for k in range(2)]
    g_tall = pl.BlockSpec((8, 1, 1, 128, H // 2), lambda i, r: (0, i, 2, 0, r))
    one = [pl.BlockSpec((1, d // 2, H), wide)] * 2 + [pl.BlockSpec((1, H // 2, d), tall)]
    given = len(so_far)
    params = count * 3 * d * H
    return pl.pallas_call(
        adam_kernel,
        name="adamw",
        grid=(count, 2),
        out_shape=[jax.ShapeDtypeStruct(t.shape, t.dtype) for t in arrays],
        in_specs=g_wide + [g_tall] + one * 3 + [pl.BlockSpec(memory_space=pl.ANY)] * given,
        out_specs=one * 3,
        input_output_aliases={12 + i: i for i in range(given)},
        compiler_params=pltpu.CompilerParams(vmem_limit_bytes=60_000_000),
        cost_estimate=pl.CostEstimate(flops=12 * params, bytes_accessed=22 * params, transcendentals=params),
    )(g, g, g, *arrays, *so_far)


def solution(mesh):
    def step(x, dy, *arrays):
        shard = gradients_of(x[0], dy[0], *arrays[:3])
        gathered, first = [], 0
        for count in GROUPS:
            gathered.append((first, count, lax.all_gather(shard[first : first + count], "dp", axis=0)))
            first += count
        so_far = ()
        for first, count, g in gathered:
            so_far = tuple(adam(first, count, g, arrays, so_far))
        return so_far

    return jax.shard_map(
        step,
        mesh=mesh,
        in_specs=(P(("rep", "dp"), None, None),) * 2 + (P(None, None, None),) * 9,
        out_specs=(P("rep", None, None),) * 9,
        check_vma=False,
    )
```
